32 devices in a mesh: swath: 8 (over y, x, core), chan: 4 (over z).
Axes of the slice: x: 2, y: 2, z: 4, core: 2. Of those that a mesh axis runs over, the one named last changes fastest.
Arguments:
- innovations: float32 [524288], P(('swath', 'chan')), may hold values from -6 to 6
- obs_precision: float32 [524288], P(('swath', 'chan')), may hold values from 0.25 to 4
- jacobian: bfloat16 [524288, 128], P(('swath', 'chan')), may hold values from -0.5 to 0.5
- predictors: float32 [8, 524288], P(None, ('swath', 'chan')), may hold values from -5 to 5
- obs_column: int32 [524288], P(('swath', 'chan')), may hold values from 0 to 2047, as said below
- obs_channel: int32 [524288], P(('swath', 'chan')), may hold values from 0 to 5119
- obs_count: int32 [8, 4], P('swath', 'chan'), may hold values from 5461 to 16384, as said below
- smoothing: float32 [128], replicated, may hold values from 0.02 to 0.12
- bias_precision: float32 [8, 5120], P(None, 'chan'), may hold values from 1 to 100
Outputs:
- control_state: float32 [256, 256, 128], P('swath', 'chan')
- bias_increment: float32 [8, 5120], P(None, 'chan')
- residual_norms: float32 [3], replicated
The draws below stay inside these ranges and needn't reach their ends.
Inputs may be any that keep to these rules, and one draw needn't show every extreme that they name: `obs_column`: Row-major index latitude row * 64 + longitude column within the tile of the device that holds the slot; all slots of an aligned block of 128 slots lie in one latitude row. `obs_channel`: channel c belongs to block c // 256, whose coefficients are owned by chan index c // 1280. `obs_count`: slots below the count hold live observations, the rest are ignored; some device is full in every draw.
All inputs are finite; a program needn't handle non-finite values.
Results may differ from the reference program's by a relative error of at most 0.0003.
Values sent between devices are 32-bit elements; how exact they have to be, the bound alone decides.
No kernel may reach another device: no remote copies, remote signals or barrier semaphores. Data moves between devices by JAX's collectives and lax.ppermute only.
A program may use at most 128 MiB of HBM per device.

```python
import math
import jax
import jax.numpy as jnp
from jax import lax

LEV = 128
NPRED = 8
OBS_BLOCK = 128
LAT_DEV = 32
LON_DEV = 64
OBS_DEV = 16384
ITERS = 2
OBS_ALL = 524288
CHANNELS = 5120
N_SWATH = 8
N_CHAN = 4


def draw_obs_count(key, part):
    devices_all = N_SWATH * N_CHAN
    counts = jax.random.randint(jax.random.fold_in(key, 11), (devices_all,), OBS_DEV // 3, OBS_DEV + 1)
    fullest = jax.random.randint(jax.random.fold_in(key, 12), (), 0, devices_all)
    counts = jnp.where(jnp.arange(devices_all) == fullest, OBS_DEV, counts)
    return counts.reshape(N_SWATH, N_CHAN).astype(jnp.int32)


def draw_obs_column(key, part):
    block_count = OBS_DEV * N_SWATH * N_CHAN // OBS_BLOCK
    line_rows = jax.random.randint(jax.random.fold_in(key, 21), (block_count,), 0, LAT_DEV)
    line_cols = jax.random.randint(jax.random.fold_in(key, 22), (block_count, OBS_BLOCK), 0, LON_DEV)
    return (line_rows[:, None] * LON_DEV + line_cols).reshape(-1).astype(jnp.int32)


def touch_ends(entries, rng, smallest, largest):
    longest = entries.shape.index(max(entries.shape))
    spots = []
    for shift in (0, 1):
        where = [jax.random.randint(jax.random.fold_in(rng, axis), (), 0, length) for axis, length in enumerate(entries.shape)]
        where[longest] = (where[longest] + shift) % entries.shape[longest]
        spots.append(tuple(where))
    return entries.at[spots[0]].set(smallest).at[spots[1]].set(largest)


def steps_of(own_key, dims, split, least, top_value):
    def one(axis_at, blocks):
        draws = jax.random.uniform(jax.random.fold_in(jax.random.fold_in(own_key, 6), axis_at), (blocks,), jnp.float32, least / len(split), top_value / len(split))
        return jnp.repeat(jnp.exp(draws), dims[axis_at] // blocks).reshape((-1,) + (1,) * (len(dims) - axis_at - 1))

    level = one(*split[0])
    for cut in split[1:]:
        level = level * one(*cut)
    return level


def centred(own_key, shape, deviation, most, pieces=(), kind=jnp.bfloat16):
    result = jax.random.normal(own_key, shape, jnp.float32) * deviation
    if len(pieces) > 0:
        result = steps_of(own_key, shape, pieces, -0.22, 0.18) * result
    return jnp.clip(result, min=-most, max=most).astype(kind)


def setup_inputs(seed: int = 0) -> dict:
    arg_keys = jax.random.split(jax.random.key(seed), 10)
    innovations = centred(arg_keys[0], (OBS_ALL,), 1.0, 6.0, ((0, 32),), jnp.float32)
    obs_precision = jnp.clip(jnp.exp(math.log(4.0) - 2.7725887 * jax.random.uniform(arg_keys[1], (OBS_ALL,), jnp.float32) ** steps_of(arg_keys[1], (OBS_ALL,), ((0, 32),), -0.2, 0.2)), 0.25, 4.0)
    jacobian = centred(arg_keys[2], (OBS_ALL, LEV), LEV ** -0.5, 0.5, ((0, 32),))
    predictors = centred(arg_keys[3], (NPRED, OBS_ALL), 1.0, 5.0, ((1, 32),), jnp.float32)
    obs_column = draw_obs_column(jax.random.fold_in(arg_keys[9], 71), 0)
    obs_channel = touch_ends(jax.random.randint(arg_keys[5], (OBS_ALL,), 0, CHANNELS), jax.random.fold_in(arg_keys[5], 1), 0, CHANNELS - 1).astype(jnp.int32)
    obs_count = draw_obs_count(jax.random.fold_in(arg_keys[9], 71), 0)
    smoothing = jnp.clip(jnp.exp(jax.random.uniform(arg_keys[7], (LEV,), jnp.float32, math.log(0.02), math.log(0.12))), 0.02, 0.12)
    bias_precision = jnp.clip(jnp.exp(math.log(100.0) - 4.6051702 * jax.random.uniform(arg_keys[8], (NPRED, CHANNELS), jnp.float32) ** steps_of(arg_keys[8], (NPRED, CHANNELS), ((1, 4),), -0.2, 0.2)), 1.0, 100.0)
    return dict(innovations=innovations, obs_precision=obs_precision, jacobian=jacobian, predictors=predictors, obs_column=obs_column, obs_channel=obs_channel, obs_count=obs_count, smoothing=smoothing, bias_precision=bias_precision)


def smooth_field(state_field, smoothing):
    padded = jnp.pad(state_field, ((1, 1), (0, 0), (0, 0)))
    beside = padded[:-2] + padded[2:] + jnp.roll(state_field, 1, axis=1) + jnp.roll(state_field, -1, axis=1)
    return state_field + smoothing * (beside - 4.0 * state_field)

def reference(innovations, obs_precision, jacobian, predictors, obs_column, obs_channel, obs_count, smoothing, bias_precision):
    devices_all = N_SWATH * N_CHAN
    lat_all = LAT_DEV * N_SWATH
    lon_all = LON_DEV * N_CHAN
    cells_all = lat_all * lon_all
    slot_ids = jnp.arange(devices_all * OBS_DEV, dtype=jnp.int32)
    holder = slot_ids // OBS_DEV
    row_index = holder // N_CHAN * LAT_DEV + obs_column // LON_DEV
    col_index = holder % N_CHAN * LON_DEV + obs_column % LON_DEV
    flat_cell = (row_index * lon_all + col_index).astype(jnp.int32)
    live = slot_ids % OBS_DEV < obs_count.reshape(-1)[holder]
    weights = jnp.where(live, obs_precision, jnp.zeros_like(obs_precision))
    jac_blocks = jacobian.reshape(devices_all, OBS_DEV, LEV)
    cell_blocks = flat_cell.reshape(devices_all, OBS_DEV)

    def forward(state_field):
        table = state_field.reshape(cells_all, LEV)

        def one_block(pair):
            return lax.optimization_barrier(jnp.sum(pair[0].astype(jnp.float32) * table[pair[1]], axis=1))
        return lax.map(one_block, (jac_blocks, cell_blocks)).reshape(-1)

    def adjoint(values):
        value_blocks = values.reshape(devices_all, OBS_DEV)

        def add_block(table, triple):
            return (table.at[triple[1]].add(triple[0].astype(jnp.float32) * triple[2][:, None]), 0)
        start_table = jnp.zeros((cells_all, LEV), jnp.float32)
        table = lax.scan(add_block, start_table, (jac_blocks, cell_blocks, value_blocks))[0]
        return table.reshape(lat_all, lon_all, LEV)

    def bias_forward(coefs):
        return lax.optimization_barrier(jnp.sum(predictors * coefs[:, obs_channel], axis=0))

    def bias_adjoint(terms):
        return jnp.zeros((NPRED, CHANNELS), jnp.float32).at[:, obs_channel].add(terms)

    def hessian(state_dir, bias_dir):
        image = weights * (forward(smooth_field(state_dir, smoothing)) + bias_forward(bias_dir))
        return (state_dir + smooth_field(adjoint(image), smoothing), bias_precision * bias_dir + bias_adjoint(predictors * image[None, :]))
    source = weights * innovations
    res_state = smooth_field(adjoint(source), smoothing)
    res_bias = bias_adjoint(predictors * source[None, :])
    diagonal = bias_precision + bias_adjoint(predictors * predictors * weights[None, :])
    sol_state = jnp.zeros_like(res_state)
    sol_bias = jnp.zeros_like(res_bias)
    pre_bias = res_bias / diagonal
    dir_state, dir_bias = (res_state, pre_bias)
    state_sq = jnp.sum(res_state * res_state)
    rz_now = state_sq + jnp.sum(res_bias * pre_bias)
    record = [state_sq + jnp.sum(res_bias * res_bias)]
    for turn_index in range(ITERS):
        img_state, img_bias = hessian(dir_state, dir_bias)
        length = rz_now / (jnp.sum(dir_state * img_state) + jnp.sum(dir_bias * img_bias))
        sol_state = sol_state + length * dir_state
        sol_bias = sol_bias + length * dir_bias
        res_state = res_state - length * img_state
        res_bias = res_bias - length * img_bias
        pre_bias = res_bias / diagonal
        state_sq = jnp.sum(res_state * res_state)
        rz_next = state_sq + jnp.sum(res_bias * pre_bias)
        record.append(state_sq + jnp.sum(res_bias * res_bias))
        ratio = rz_next / rz_now
        dir_state = res_state + ratio * dir_state
        dir_bias = pre_bias + ratio * dir_bias
        rz_now = rz_next
    return (sol_state, sol_bias, jnp.sqrt(jnp.stack(record)))
```

```python
import functools
import jax
import jax.numpy as jnp
from jax import lax
from jax.experimental import pallas as pl
from jax.experimental.pallas import tpu as pltpu
from jax.sharding import PartitionSpec as P

LEV = 128
NPRED = 8
CH_BLOCK = 256
OBS_BLOCK = 128
LAT_DEV = 32
LON_DEV = 64
GROUP = 8
PAD = 8
SHRINK = 2.0 ** -16
F32 = jnp.float32
BF16 = jnp.bfloat16
VMEM = pl.BlockSpec(memory_space=pltpu.VMEM)
SMEM = pl.BlockSpec(memory_space=pltpu.SMEM)
NT = (((1,), (1,)), ((), ()))


def two_parts(value):
    high = value.astype(BF16)
    low = (value - high.astype(F32)).astype(BF16)
    return high, low


def dot(one, two, dims=(((1,), (0,)), ((), ()))):
    return lax.dot_general(one, two, dims, preferred_element_type=F32)


def channel_hot(channel):
    rows = lax.broadcasted_iota(jnp.int32, (CH_BLOCK, OBS_BLOCK), 0)
    cols = []
    for line in range(GROUP):
        inner = jnp.bitwise_and(channel[line : line + 1], CH_BLOCK - 1)
        cols.append(jnp.where(rows == inner, 1.0, 0.0).astype(BF16))
    return jnp.concatenate(cols, axis=1)


def flat_lines(value):
    return jnp.concatenate([value[line : line + 1] for line in range(GROUP)], axis=1)


def spread(terms, block_row, blocks):
    high, low = two_parts(terms)
    pieces = jnp.concatenate([high, low], axis=0)
    wide = jnp.broadcast_to(block_row, pieces.shape)
    zero = jnp.zeros_like(pieces)
    return jnp.concatenate(
        [jnp.where(wide == float(b), pieces, zero) for b in range(blocks)], axis=0
    )


def put_table(out_ref, acc_ref, blocks, added):
    for b in range(blocks):
        at = slice(b * CH_BLOCK, (b + 1) * CH_BLOCK)
        low = 2 * NPRED * b
        total = acc_ref[low : low + NPRED] + acc_ref[low + NPRED : low + 2 * NPRED]
        out_ref[:, at] = total + added(at)


def first_bias_kernel(
    count_ref, innov_ref, prec_ref, chan_ref, pred_ref, prior_ref,
    source_ref, weight_ref, table_ref, diag_ref, acc_ref, dacc_ref,
):
    lines = innov_ref.shape[0]
    blocks = acc_ref.shape[0] // (2 * NPRED)
    acc_ref[...] = jnp.zeros_like(acc_ref)
    dacc_ref[...] = jnp.zeros_like(dacc_ref)

    def step(i, _):
        at = pl.ds(pl.multiple_of(i * GROUP, GROUP), GROUP)
        wide = pl.ds(pl.multiple_of(i * GROUP * OBS_BLOCK, GROUP * OBS_BLOCK), GROUP * OBS_BLOCK)
        slot = (
            (i * GROUP + lax.broadcasted_iota(jnp.int32, (GROUP, OBS_BLOCK), 0)) * OBS_BLOCK
            + lax.broadcasted_iota(jnp.int32, (GROUP, OBS_BLOCK), 1)
        )
        weight = jnp.where(slot < count_ref[0, 0], prec_ref[at], 0.0)
        source = weight * innov_ref[at]
        weight_ref[at] = weight
        source_ref[at] = source
        channel = chan_ref[at]
        hot = channel_hot(channel)
        block_row = flat_lines(lax.shift_right_logical(channel, 8).astype(F32)).astype(BF16)
        pred = pred_ref[:, wide]
        acc_ref[...] += dot(spread(pred * flat_lines(source), block_row, blocks), hot, NT)
        dacc_ref[...] += dot(spread(pred * pred * flat_lines(weight), block_row, blocks), hot, NT)
        return 0

    lax.fori_loop(0, lines // GROUP, step, 0)
    put_table(table_ref, acc_ref, blocks, lambda at: 0.0)
    put_table(diag_ref, dacc_ref, blocks, lambda at: prior_ref[:, at])


def bias_kernel(
    image_ref, weight_ref, chan_ref, pred_ref, coef_ref, prior_ref,
    value_ref, table_ref, acc_ref, look_ref,
):
    lines = image_ref.shape[0]
    blocks = acc_ref.shape[0] // (2 * NPRED)
    acc_ref[...] = jnp.zeros_like(acc_ref)
    for b in range(blocks):
        high, low = two_parts(coef_ref[:, b * CH_BLOCK : (b + 1) * CH_BLOCK])
        look_ref[2 * NPRED * b : 2 * NPRED * (b + 1)] = jnp.concatenate([high, low], axis=0)

    def step(i, _):
        at = pl.ds(pl.multiple_of(i * GROUP, GROUP), GROUP)
        wide = pl.ds(pl.multiple_of(i * GROUP * OBS_BLOCK, GROUP * OBS_BLOCK), GROUP * OBS_BLOCK)
        channel = chan_ref[at]
        hot = channel_hot(channel)
        block_f32 = flat_lines(lax.shift_right_logical(channel, 8).astype(F32))
        pred = pred_ref[:, wide]
        found = dot(look_ref[...], hot)
        block_wide = jnp.broadcast_to(block_f32, pred.shape)
        picked = jnp.zeros_like(pred)
        for b in range(blocks):
            low = 2 * NPRED * b
            both = found[low : low + NPRED] + found[low + NPRED : low + 2 * NPRED]
            picked = jnp.where(block_wide == float(b), both, picked)
        looked = jnp.sum(picked * pred, axis=0, keepdims=True)
        value = flat_lines(weight_ref[at]) * (flat_lines(image_ref[at]) + looked)
        value_ref[at] = jnp.concatenate(
            [value[:, j * OBS_BLOCK : (j + 1) * OBS_BLOCK] for j in range(GROUP)], axis=0
        )
        acc_ref[...] += dot(spread(pred * value, block_f32.astype(BF16), blocks), hot, NT)
        return 0

    lax.fori_loop(0, lines // GROUP, step, 0)
    put_table(table_ref, acc_ref, blocks, lambda at: prior_ref[:, at] * coef_ref[:, at])


def adjoint_kernel(scale, has_base, row_ref, value_ref, col_ref, jac_ref, *rest):
    if has_base:
        base_ref, out_ref = rest
        out_ref[...] = base_ref[...]
    else:
        (out_ref,) = rest
        out_ref[...] = jnp.zeros_like(out_ref)
    lines = value_ref.shape[0]
    cells = lax.broadcasted_iota(jnp.int32, (LON_DEV, OBS_BLOCK), 0)

    def step(i, _):
        at = pl.ds(pl.multiple_of(i * GROUP, GROUP), GROUP)
        value = value_ref[at]
        high = value.astype(BF16).astype(F32)
        low = value - high
        col = jnp.bitwise_and(col_ref[at], LON_DEV - 1)
        for j in range(GROUP):
            hit = cells == col[j : j + 1]
            left = jnp.concatenate(
                [jnp.where(hit, high[j : j + 1], 0.0), jnp.where(hit, low[j : j + 1], 0.0)], axis=0
            ).astype(BF16)
            line = i * GROUP + j
            jac = jac_ref[pl.ds(pl.multiple_of(line * OBS_BLOCK, OBS_BLOCK), OBS_BLOCK), :]
            got = dot(left, jac)
            row = row_ref[line]
            out_ref[row] += got[:LON_DEV] + got[LON_DEV:]
        return 0

    lax.fori_loop(0, lines // GROUP, step, 0)
    if scale != 1.0:
        out_ref[...] = out_ref[...] * scale


def fill_padded(pad_ref, g_ref, up_ref, down_ref, west_ref, east_ref, width):
    rows = g_ref.shape[0]
    pad_ref[width : width + rows, PAD : PAD + LON_DEV] = g_ref[...]
    pad_ref[0:width, PAD : PAD + LON_DEV] = up_ref[...]
    pad_ref[width + rows : 2 * width + rows, PAD : PAD + LON_DEV] = down_ref[...]
    pad_ref[:, PAD - width : PAD] = west_ref[...]
    pad_ref[:, PAD + LON_DEV : PAD + LON_DEV + width] = east_ref[...]


def smoothed_row(pad_ref, row, smooth):
    here = pad_ref[row]
    size = here.shape[0]
    beside = (
        pad_ref[row - 1]
        + pad_ref[row + 1]
        + pltpu.roll(here, 1, 0)
        + pltpu.roll(here, size - 1, 0)
    )
    return here + smooth * (beside - 4.0 * here)


def forward_kernel(
    row_ref, keep_ref, smooth_ref, g_ref, up_ref, down_ref, west_ref, east_ref, col_ref, jac_ref,
    image_ref, z_ref, pad_ref, zpad_ref, part_ref,
):
    rows = g_ref.shape[0]
    lines = col_ref.shape[0]
    smooth = smooth_ref[...]
    fill_padded(pad_ref, g_ref, up_ref, down_ref, west_ref, east_ref, 2)

    def first(r, _):
        zpad_ref[r] = smoothed_row(pad_ref, r + 1, smooth)
        return 0

    lax.fori_loop(0, rows + 2, first, 0)

    @pl.when(keep_ref[0] == 0)
    def _():
        zpad_ref[0] = jnp.zeros_like(zpad_ref[0])

    @pl.when(keep_ref[1] == 0)
    def _():
        zpad_ref[rows + 1] = jnp.zeros_like(zpad_ref[0])

    z_ref[...] = zpad_ref[1 : rows + 1, PAD : PAD + LON_DEV]

    def second(r, _):
        high, low = two_parts(smoothed_row(zpad_ref, r + 1, smooth)[PAD : PAD + LON_DEV])
        part_ref[r] = jnp.concatenate([high, low], axis=0)
        return 0

    lax.fori_loop(0, rows, second, 0)
    cells = lax.broadcasted_iota(jnp.int32, (LON_DEV, OBS_BLOCK), 0)

    def step(i, _):
        at = pl.ds(pl.multiple_of(i * GROUP, GROUP), GROUP)
        col = jnp.bitwise_and(col_ref[at], LON_DEV - 1)
        found = []
        for j in range(GROUP):
            line = i * GROUP + j
            jac = jac_ref[pl.ds(pl.multiple_of(line * OBS_BLOCK, OBS_BLOCK), OBS_BLOCK), :]
            got = dot(part_ref[row_ref[line]], jac, NT)
            both = got[:LON_DEV] + got[LON_DEV:]
            found.append(
                jnp.sum(jnp.where(cells == col[j : j + 1], both, 0.0), axis=0, keepdims=True)
            )
        image_ref[at] = jnp.concatenate(found, axis=0)
        return 0

    lax.fori_loop(0, lines // GROUP, step, 0)


def gram_kernel(
    lead_ref, smooth_ref, g_ref, up_ref, down_ref, west_ref, east_ref, z_ref, w_ref,
    rb_ref, zb_ref, wb_ref, ub_ref, vb_ref, sum_ref, pad_ref,
):
    rows = g_ref.shape[0]
    smooth = smooth_ref[...]
    fill_padded(pad_ref, g_ref, up_ref, down_ref, west_ref, east_ref, 1)

    def step(r, sums):
        z = z_ref[r]
        w = w_ref[r]
        v = smoothed_row(pad_ref, r + 1, smooth)[PAD : PAD + LON_DEV]
        made = []
        for total, (one, two) in zip(sums, ((z, z), (z, w), (w, w), (z, v), (w, v), (v, v))):
            made.append(total + jnp.sum((one * two).reshape(LON_DEV // 8, 8, LEV), axis=0))
        return tuple(made)

    zero = jnp.zeros((8, LEV), F32)
    zz, zw, ww, zv, wv, vv = lax.fori_loop(0, rows, step, (zero,) * 6)
    lead = jnp.where(lead_ref[0] > 0, 1.0, 0.0)
    rb, zb, wb, ub, vb = (ref[...] for ref in (rb_ref, zb_ref, wb_ref, ub_ref, vb_ref))

    def both(state, one, two):
        a = jnp.sum(state, axis=0, keepdims=True)
        b = jnp.sum(jnp.sum(one * two, axis=0, keepdims=True), axis=1, keepdims=True) * lead
        return a + b * (1.0 / LEV)

    sums = [
        both(zz, rb, rb), both(zz, rb, zb), both(zw, zb, wb), both(zw, rb, wb),
        both(ww, wb, ub), both(ww, wb, wb), both(wv, ub, vb), both(zv, rb, vb),
        both(wv, wb, vb), both(vv, vb, vb),
    ]
    sums += [jnp.zeros_like(sums[0])] * (16 - len(sums))
    sum_ref[...] = jnp.concatenate(sums, axis=0)


def final_kernel(count, *refs):
    ins = refs[:count]
    z_ref, w_ref, zb_ref, ub_ref, x_ref, xb_ref, norm_ref = refs[count:]
    total = ins[0][...]
    for ref in ins[1:]:
        total = total + ref[...]
    total = jnp.sum(total, axis=1, keepdims=True)
    rr, rz, zw, rw, wu, ww, uv, rv, wv, vv = (total[i : i + 1] for i in range(10))
    grow = 1.0 / SHRINK
    first = rz / (zw * grow)
    big = first * grow
    rz_one = rz - 2.0 * big * zw + big * big * wu
    rr_one = rr - 2.0 * big * rw + big * big * ww
    ratio = rz_one / rz
    lift = 1.0 + ratio
    curve = lift * lift * (zw * grow) - 2.0 * lift * first * wu * (grow * grow) + big * big * uv
    second = rz_one / curve
    main = first + second * lift
    side = first * second * grow
    main_big = main * grow
    rr_two = (
        rr + main_big * main_big * ww + side * side * vv
        - 2.0 * main_big * rw + 2.0 * side * rv - 2.0 * main_big * side * wv
    )
    x_ref[...] = main[:, None] * z_ref[...] - side[:, None] * w_ref[...]
    xb_ref[...] = main * zb_ref[...] - side * ub_ref[...]
    lane = lax.broadcasted_iota(jnp.int32, (8, LEV), 1)
    squares = jnp.where(lane == 0, rr, jnp.where(lane == 1, rr_one, rr_two))
    norm_ref[...] = jnp.sqrt(jnp.maximum(squares, 0.0))


def call(kernel, outs, scratch=(), flops=0, spaces=None, count=None, name=None):
    shapes = [jax.ShapeDtypeStruct(s, d) for s, d in outs]

    def run(*args):
        specs = [SMEM if i in (spaces or ()) else VMEM for i in range(len(args))]
        return pl.pallas_call(
            kernel,
            out_shape=shapes,
            in_specs=specs,
            out_specs=[VMEM] * len(shapes),
            scratch_shapes=list(scratch),
            cost_estimate=pl.CostEstimate(flops=flops, transcendentals=0, bytes_accessed=1 << 20),
            name=name,
            compiler_params=pltpu.CompilerParams(vmem_limit_bytes=48 << 20),
        )(*args)

    return run


def trade(value, axis, mask):
    size = lax.axis_size(axis)
    return lax.ppermute(value, axis, [(i, i ^ mask) for i in range(size)])


def scatter_rows(tables):
    size = lax.axis_size("swath")
    index = lax.axis_index("swath")
    table = jnp.concatenate(tables, axis=0)
    half = table.shape[1] // 2
    odd = index % 2
    mine = lax.dynamic_slice_in_dim(table, odd * half, half, 1)
    other = lax.dynamic_slice_in_dim(table, (1 - odd) * half, half, 1)
    mine = mine + trade(other, "swath", 1)
    place = index // 2
    width = half // (size // 2)
    own = lax.dynamic_slice_in_dim(mine, place * width, width, 1)
    got = [
        trade(lax.dynamic_slice_in_dim(mine, (place ^ m) * width, width, 1), "swath", 2 * m)
        for m in range(1, size // 2)
    ]
    for piece in got:
        own = own + piece
    return own


def sum_sectors(own):
    got = [trade(own, "chan", m) for m in range(1, lax.axis_size("chan"))]
    for piece in got:
        own = own + piece
    return own


def gather_rows(own):
    size = lax.axis_size("swath")
    index = lax.axis_index("swath")
    place = index // 2
    odd = index % 2
    width = own.shape[1]
    mine = jnp.zeros((own.shape[0], width * (size // 2)), own.dtype)
    mine = lax.dynamic_update_slice_in_dim(mine, own, place * width, 1)
    got = [trade(own, "swath", 2 * m) for m in range(1, size // 2)]
    for m, piece in enumerate(got, 1):
        mine = lax.dynamic_update_slice_in_dim(mine, piece, (place ^ m) * width, 1)
    other = trade(mine, "swath", 1)
    low = jnp.where(odd == 0, mine, other)
    high = jnp.where(odd == 0, other, mine)
    return jnp.concatenate([low, high], axis=1)


def halos(g, width):
    rows, cols = g.shape[0], g.shape[1]
    bands = lax.axis_size("swath")
    sectors = lax.axis_size("chan")
    up = lax.ppermute(g[rows - width :], "swath", [(i, i + 1) for i in range(bands - 1)])
    down = lax.ppermute(g[:width], "swath", [(i + 1, i) for i in range(bands - 1)])
    tall = lambda cut: jnp.concatenate([up[:, cut], g[:, cut], down[:, cut]], axis=0)
    west = lax.ppermute(
        tall(slice(cols - width, cols)), "chan", [(i, (i + 1) % sectors) for i in range(sectors)]
    )
    east = lax.ppermute(
        tall(slice(0, width)), "chan", [((i + 1) % sectors, i) for i in range(sectors)]
    )
    return up, down, west, east


def body(
    innovations, obs_precision, jacobian, predictors, obs_column, obs_channel, obs_count,
    smoothing, bias_precision,
):
    slots = obs_precision.shape[0]
    lines = slots // OBS_BLOCK
    owned = bias_precision.shape[1]
    channels = owned * lax.axis_size("chan")
    blocks = channels // CH_BLOCK
    band = lax.axis_index("swath")
    sector = lax.axis_index("chan")
    keep = jnp.stack([band > 0, band < lax.axis_size("swath") - 1]).astype(jnp.int32)
    lead = (sector == 0).astype(jnp.int32).reshape(1)
    smooth = smoothing.reshape(1, LEV)
    by_line = (lines, OBS_BLOCK)
    col = obs_column.reshape(by_line)
    channel = obs_channel.reshape(by_line)
    rows = col[:, 0] // LON_DEV
    prior = lax.dynamic_update_slice_in_dim(
        jnp.zeros((NPRED, channels), F32),
        jnp.where(band == 0, bias_precision, 0.0),
        sector * owned,
        1,
    )
    tile = (LAT_DEV, LON_DEV, LEV)
    table = (NPRED, channels)
    wide = LON_DEV + 2 * PAD
    acc = pltpu.VMEM((2 * NPRED * blocks, CH_BLOCK), F32)
    hot_flops = 2 * 2 * NPRED * blocks * CH_BLOCK * slots
    tile_flops = 4 * LON_DEV * LEV * slots
    line_out = (by_line, F32)

    first_bias = call(
        first_bias_kernel, [line_out, line_out, (table, F32), (table, F32)], [acc, acc],
        2 * hot_flops, (0,), name="first_bias",
    )
    bias = call(
        bias_kernel, [line_out, (table, F32)],
        [acc, pltpu.VMEM((2 * NPRED * blocks, CH_BLOCK), BF16)], 2 * hot_flops, name="bias",
    )

    def adjoint(value, base, scale):
        kernel = functools.partial(adjoint_kernel, scale, base is not None)
        args = (rows, value, col, jacobian) + (() if base is None else (base,))
        return call(kernel, [(tile, F32)], (), tile_flops, (0,), name="adjoint")(*args)[0]

    forward = call(
        forward_kernel, [line_out, (tile, F32)],
        [
            pltpu.VMEM((LAT_DEV + 4, wide, LEV), F32),
            pltpu.VMEM((LAT_DEV + 2, wide, LEV), F32),
            pltpu.VMEM((LAT_DEV, 2 * LON_DEV, LEV), BF16),
        ],
        tile_flops, (0, 1), name="forward",
    )
    gram = call(
        gram_kernel, [((16, LEV), F32)], [pltpu.VMEM((LAT_DEV + 2, wide, LEV), F32)],
        1 << 22, (0,), name="gram",
    )

    source, weight, table0, diag0 = first_bias(
        obs_count, innovations.reshape(by_line), obs_precision.reshape(by_line), channel,
        predictors, prior,
    )
    both = scatter_rows([table0, diag0])
    g0 = adjoint(source, None, 1.0)
    both = sum_sectors(both)
    rb, diag = both[:NPRED], both[NPRED:]
    zb = rb / diag
    z_all = gather_rows(zb)
    image, z = forward(rows, keep, smooth, g0, *halos(g0, 2), col, jacobian)
    value, table1 = bias(image, weight, channel, predictors, z_all, prior)
    wb = scatter_rows([table1])
    g1 = adjoint(value, g0, SHRINK)
    wb = sum_sectors(wb) * SHRINK
    ub = wb / diag
    u_all = gather_rows(ub)
    image, w = forward(rows, keep, smooth, g1, *halos(g1, 2), col, jacobian)
    value, table2 = bias(image, weight, channel, predictors, u_all, prior)
    vb = scatter_rows([table2])
    g2 = adjoint(value, g1, 1.0)
    vb = sum_sectors(vb)
    sums = gram(lead, smooth, g2, *halos(g2, 1), z, w, rb, zb, wb, ub, vb)[0]
    sums = sums + trade(sums, "swath", 1)
    got = [trade(sums, "swath", 2 * m) for m in range(1, lax.axis_size("swath") // 2)]
    for piece in got:
        sums = sums + piece
    got = [sums] + [trade(sums, "chan", m) for m in range(1, lax.axis_size("chan"))]
    own_z = lax.dynamic_slice_in_dim(z_all, sector * owned, owned, 1)
    own_u = lax.dynamic_slice_in_dim(u_all, sector * owned, owned, 1)
    x, xb, norms = call(
        functools.partial(final_kernel, len(got)),
        [(tile, F32), ((NPRED, owned), F32), ((8, LEV), F32)], name="final",
    )(*got, z, w, own_z, own_u)
    return x, xb, norms[0, :3]


def solution(mesh):
    placed = (
        P(("swath", "chan")),
        P(("swath", "chan")),
        P(("swath", "chan"), None),
        P(None, ("swath", "chan")),
        P(("swath", "chan")),
        P(("swath", "chan")),
        P("swath", "chan"),
        P(),
        P(None, "chan"),
    )
    return jax.shard_map(
        body,
        mesh=mesh,
        in_specs=placed,
        out_specs=(P("swath", "chan", None), P(None, "chan"), P()),
        check_vma=False,
    )
```

```python
import functools
import jax
import jax.numpy as jnp
from jax import lax
from jax.experimental import pallas as pl
from jax.experimental.pallas import tpu as pltpu
from jax.sharding import PartitionSpec as P


LEV = 128
NPRED = 8
CH_BLOCK = 256
OBS_BLOCK = 128
LAT_DEV = 32
LON_DEV = 64
GROUP = 8
PAD = 8
UNROLL = 2
LANES = 128
SPLIT = CH_BLOCK // LANES
SHRINK = 2.0 ** -16
F32 = jnp.float32
BF16 = jnp.bfloat16
VMEM = pl.BlockSpec(memory_space=pltpu.VMEM)
SMEM = pl.BlockSpec(memory_space=pltpu.SMEM)
HBM = pl.BlockSpec(memory_space=pltpu.HBM)
NT = (((1,), (1,)), ((), ()))


def two_parts(value):
    high = value.astype(BF16)
    low = (value - high.astype(F32)).astype(BF16)
    return high, low


def dot(one, two, dims=(((1,), (0,)), ((), ()))):
    return lax.dot_general(one, two, dims, preferred_element_type=F32)


def channel_hot(channel):
    rows = lax.broadcasted_iota(jnp.int32, (CH_BLOCK, OBS_BLOCK), 0).astype(F32).astype(BF16)
    inner = jnp.bitwise_and(channel, CH_BLOCK - 1).astype(F32).astype(BF16)
    one, zero = jnp.ones_like(rows), jnp.zeros_like(rows)
    return jnp.concatenate(
        [jnp.where(rows == inner[line : line + 1], one, zero) for line in range(GROUP)], axis=1
    )


def flat_lines(value):
    return jnp.concatenate([value[line : line + 1] for line in range(GROUP)], axis=1)


def spread(terms, block_row, blocks):
    high, low = two_parts(terms)
    pieces = jnp.concatenate([high, low], axis=0)
    wide = jnp.broadcast_to(block_row, pieces.shape)
    zero = jnp.zeros_like(pieces)
    return jnp.concatenate(
        [jnp.where(wide == float(b), pieces, zero) for b in range(blocks)], axis=0
    )


def give_halves(full, mine_ref, other_ref):
    half = mine_ref.shape[0]
    odd = lax.axis_index("swath") % 2
    mine_ref[...] = full[pl.ds(odd * half, half)]
    other_ref[...] = full[pl.ds((1 - odd) * half, half)]


def put_table(out_ref, acc_ref, blocks, added):
    for b in range(blocks):
        low = 2 * NPRED * b
        total = acc_ref[low : low + NPRED] + acc_ref[low + NPRED : low + 2 * NPRED]
        for h in range(SPLIT):
            unit = SPLIT * b + h
            out_ref[unit] = total[:, h * LANES : (h + 1) * LANES] + added(unit)


def fetch(pairs, sems):
    copies = [pltpu.make_async_copy(a, b, sems.at[i]) for i, (a, b) in enumerate(pairs)]
    for copy in copies:
        copy.start()
    return copies


def chunk_copy(hbm_ref, ref, sems, i, size, axis):
    at = pl.ds(pl.multiple_of(i * size, size), size)
    where = at if axis == 0 else (slice(None), at)
    return pltpu.make_async_copy(hbm_ref.at[where], ref.at[where], sems.at[i])


def first_bias_kernel(
    count_ref, innov_hbm, prec_hbm, own_hbm, chan_hbm, col_hbm, pred_hbm,
    source_ref, weight_ref, mine_ref, other_ref, prior_ref, chan_ref, col_ref, pred_ref,
    both_ref, acc_ref, innov_ref, prec_ref, own_ref, sems, pred_sems,
):
    lines = innov_ref.shape[0]
    blocks = acc_ref.shape[0] // (4 * NPRED)
    wide_size = GROUP * OBS_BLOCK
    copies = fetch(
        [(chan_hbm, chan_ref), (innov_hbm, innov_ref), (prec_hbm, prec_ref), (own_hbm, own_ref)], sems
    )

    def start(i, _):
        chunk_copy(pred_hbm, pred_ref, pred_sems, i, wide_size, 1).start()
        return 0

    lax.fori_loop(0, lines // GROUP, start, 0)
    late = [pltpu.make_async_copy(col_hbm, col_ref, sems.at[4])]
    for copy in late:
        copy.start()
    acc_ref[...] = jnp.zeros_like(acc_ref)
    prior_ref[...] = jnp.zeros_like(prior_ref)
    for copy in copies:
        copy.wait()

    @pl.when(lax.axis_index("swath") == 0)
    def _():
        units = own_ref.shape[1] // LANES
        for j in range(units):
            prior_ref[lax.axis_index("chan") * units + j] = own_ref[:, j * LANES : (j + 1) * LANES]

    def step(i, _):
        chunk_copy(pred_hbm, pred_ref, pred_sems, i, wide_size, 1).wait()
        at = pl.ds(pl.multiple_of(i * GROUP, GROUP), GROUP)
        wide = pl.ds(pl.multiple_of(i * wide_size, wide_size), wide_size)
        slot = (
            (i * GROUP + lax.broadcasted_iota(jnp.int32, (GROUP, OBS_BLOCK), 0)) * OBS_BLOCK
            + lax.broadcasted_iota(jnp.int32, (GROUP, OBS_BLOCK), 1)
        )
        weight = jnp.where(slot < count_ref[0, 0], prec_ref[at], 0.0)
        source = weight * innov_ref[at]
        weight_ref[at] = weight
        source_ref[at] = source
        channel = chan_ref[at]
        hot = channel_hot(channel)
        block_row = flat_lines(lax.shift_right_logical(channel, 8).astype(F32)).astype(BF16)
        pred = pred_ref[:, wide]
        terms = spread(pred * flat_lines(source), block_row, blocks)
        squares = spread(pred * pred * flat_lines(weight), block_row, blocks)
        acc_ref[...] += dot(jnp.concatenate([terms, squares], axis=0), hot, NT)
        return 0

    lax.fori_loop(0, lines // GROUP, step, 0)
    put_table(both_ref.at[0], acc_ref, blocks, lambda unit: 0.0)
    put_table(both_ref.at[1], acc_ref.at[pl.ds(2 * NPRED * blocks, 2 * NPRED * blocks)], blocks, lambda unit: prior_ref[unit])
    for k in range(2):
        give_halves(both_ref.at[k], mine_ref.at[k], other_ref.at[k])
    for copy in late:
        copy.wait()


def bias_kernel(
    image_ref, weight_ref, prior_ref, mine_ref, other_ref, chan_ref, pred_ref,
    value_ref, keep_ref, send_ref, table_ref, acc_ref, look_ref, full_ref,
):
    lines = image_ref.shape[0]
    blocks = acc_ref.shape[0] // (2 * NPRED)
    wide_size = GROUP * OBS_BLOCK
    acc_ref[...] = jnp.zeros_like(acc_ref)
    half = mine_ref.shape[0]
    odd = lax.axis_index("swath") % 2
    full_ref[pl.ds(odd * half, half)] = mine_ref[...]
    full_ref[pl.ds((1 - odd) * half, half)] = other_ref[...]
    for b in range(blocks):
        coef = jnp.concatenate([full_ref[SPLIT * b + h] for h in range(SPLIT)], axis=1)
        high, low = two_parts(coef)
        look_ref[2 * NPRED * b : 2 * NPRED * (b + 1)] = jnp.concatenate([high, low], axis=0)

    def at(i):
        return pl.ds(pl.multiple_of(i * GROUP, GROUP), GROUP)

    def wide(i):
        return pl.ds(pl.multiple_of(i * wide_size, wide_size), wide_size)

    def block_of(channel):
        return flat_lines(lax.shift_right_logical(channel, 8).astype(F32))

    def look(i):
        channel = chan_ref[at(i)]
        pred = pred_ref[:, wide(i)]
        found = dot(look_ref[...], channel_hot(channel))
        block_wide = jnp.broadcast_to(block_of(channel), pred.shape)
        picked = jnp.zeros_like(pred)
        for b in range(blocks):
            low = 2 * NPRED * b
            both = found[low : low + NPRED] + found[low + NPRED : low + 2 * NPRED]
            picked = jnp.where(block_wide == float(b), both, picked)
        looked = jnp.sum(picked * pred, axis=0, keepdims=True)
        looked = jnp.concatenate(
            [looked[:, j * OBS_BLOCK : (j + 1) * OBS_BLOCK] for j in range(GROUP)], axis=0
        )
        value = weight_ref[at(i)] * (image_ref[at(i)] + looked)
        value_ref[at(i)] = value
        return value

    def tell(i, value):
        channel = chan_ref[at(i)]
        terms = pred_ref[:, wide(i)] * flat_lines(value)
        spreads = spread(terms, block_of(channel).astype(BF16), blocks)
        acc_ref[...] += dot(spreads, channel_hot(channel), NT)

    def step(i, value):
        following = look(i)
        tell(i - 1, value)
        return following

    last = lines // GROUP - 1
    tell(last, lax.fori_loop(1, last + 1, step, look(0)))
    put_table(table_ref, acc_ref, blocks, lambda unit: prior_ref[unit] * full_ref[unit])
    give_halves(table_ref, keep_ref, send_ref)


def add_kernel(one_ref, two_ref, out_ref):
    out_ref[...] = one_ref[...] + two_ref[...]


def split_add_kernel(mask, one_ref, two_ref, keep_ref, send_ref):
    half = keep_ref.shape[0]
    bit = (lax.axis_index("swath") // mask) % 2
    keep, send = pl.ds(bit * half, half), pl.ds((1 - bit) * half, half)
    keep_ref[...] = one_ref[keep] + two_ref[keep]
    send_ref[...] = one_ref[send] + two_ref[send]


def first_ratio_kernel(one_ref, two_ref, r_ref, diag_ref, z_ref):
    r = one_ref[0] + two_ref[0]
    diag = one_ref[1] + two_ref[1]
    r_ref[...] = r
    diag_ref[...] = diag
    z_ref[...] = r / diag


def ratio_kernel(one_ref, two_ref, diag_ref, w_ref, u_ref):
    w = (one_ref[...] + two_ref[...]) * SHRINK
    w_ref[...] = w
    u_ref[...] = w / diag_ref[...]


def start_jac(jac_hbm, jac_ref, sems):
    def start(i, _):
        chunk_copy(jac_hbm, jac_ref, sems, i, GROUP * OBS_BLOCK, 0).start()
        return 0

    lax.fori_loop(0, jac_ref.shape[0] // (GROUP * OBS_BLOCK), start, 0)


def adjoint_kernel(scale, has_base, width, first, last, row_ref, value_ref, col_ref, jac_ref, *rest):
    out_ref = rest[-3] if width else rest[-1]
    if not has_base:
        out_ref[...] = jnp.zeros_like(out_ref)
    cells = lax.broadcasted_iota(jnp.int32, (LON_DEV, OBS_BLOCK), 0)

    def step(i, _):
        at = pl.ds(pl.multiple_of(i * GROUP, GROUP), GROUP)
        value = value_ref[at]
        high = value.astype(BF16).astype(F32)
        low = value - high
        col = jnp.bitwise_and(col_ref[at], LON_DEV - 1)
        for j in range(GROUP):
            hit = cells == col[j : j + 1]
            left = jnp.concatenate(
                [jnp.where(hit, high[j : j + 1], 0.0), jnp.where(hit, low[j : j + 1], 0.0)], axis=0
            ).astype(BF16)
            line = i * GROUP + j
            jac = jac_ref[pl.ds(pl.multiple_of(line * OBS_BLOCK, OBS_BLOCK), OBS_BLOCK), :]
            got = dot(left, jac)
            row = row_ref[line]
            out_ref[row] += got[:LON_DEV] + got[LON_DEV:]
        return 0

    lax.fori_loop(first, last, step, 0, unroll=UNROLL)
    if scale != 1.0:
        out_ref[...] = out_ref[...] * scale
    if width:
        near_ref, far_ref = rest[-2:]
        odd = lax.axis_index("swath") % 2 == 1
        count = out_ref.shape[0]

        @pl.when(odd)
        def _():
            near_ref[...] = out_ref[:width]
            far_ref[...] = out_ref[count - width :]

        @pl.when(jnp.logical_not(odd))
        def _():
            near_ref[...] = out_ref[count - width :]
            far_ref[...] = out_ref[:width]

        band = lax.axis_index("swath")

        @pl.when((band == 0) | (band == lax.axis_size("swath") - 1))
        def _():
            far_ref[...] = jnp.zeros_like(far_ref)


def edge_kernel(g_ref, near_ref, far_ref, beside_ref, across_ref):
    rows, width = g_ref.shape[0], near_ref.shape[0]
    left, right = slice(0, width), slice(LON_DEV - width, LON_DEV)
    odd_band = lax.axis_index("swath") % 2 == 1
    odd_sector = lax.axis_index("chan") % 2 == 1

    def put(ref, cut):
        ref[width : width + rows] = g_ref[:, cut]

        @pl.when(odd_band)
        def _():
            ref[:width] = near_ref[:, cut]
            ref[width + rows :] = far_ref[:, cut]

        @pl.when(jnp.logical_not(odd_band))
        def _():
            ref[:width] = far_ref[:, cut]
            ref[width + rows :] = near_ref[:, cut]

    @pl.when(odd_sector)
    def _():
        put(beside_ref, left)
        put(across_ref, right)

    @pl.when(jnp.logical_not(odd_sector))
    def _():
        put(beside_ref, right)
        put(across_ref, left)


def fill_padded(pad_ref, g_ref, near_ref, far_ref, beside_ref, across_ref, width):
    rows = g_ref.shape[0]
    inside = slice(PAD, PAD + LON_DEV)
    above, below = slice(0, width), slice(width + rows, 2 * width + rows)
    west, east = slice(PAD - width, PAD), slice(PAD + LON_DEV, PAD + LON_DEV + width)
    pad_ref[width : width + rows, inside] = g_ref[...]
    odd_band = lax.axis_index("swath") % 2 == 1
    odd_sector = lax.axis_index("chan") % 2 == 1

    @pl.when(odd_band)
    def _():
        pad_ref[above, inside] = near_ref[...]
        pad_ref[below, inside] = far_ref[...]

    @pl.when(jnp.logical_not(odd_band))
    def _():
        pad_ref[above, inside] = far_ref[...]
        pad_ref[below, inside] = near_ref[...]

    @pl.when(odd_sector)
    def _():
        pad_ref[:, west] = beside_ref[...]
        pad_ref[:, east] = across_ref[...]

    @pl.when(jnp.logical_not(odd_sector))
    def _():
        pad_ref[:, west] = across_ref[...]
        pad_ref[:, east] = beside_ref[...]


def smoothed_row(pad_ref, row, smooth):
    here = pad_ref[row]
    size = here.shape[0]
    beside = (
        pad_ref[row - 1]
        + pad_ref[row + 1]
        + pltpu.roll(here, 1, 0)
        + pltpu.roll(here, size - 1, 0)
    )
    return here + smooth * (beside - 4.0 * here)


def forward_kernel(
    row_ref, smooth_ref, g_ref, near_ref, far_ref, beside_ref, across_ref, col_ref, jac_hbm,
    image_ref, z_ref, pad_ref, zpad_ref, part_ref, jac_ref, sems,
):
    rows = g_ref.shape[0]
    lines = col_ref.shape[0]
    smooth = smooth_ref[...]
    start_jac(jac_hbm, jac_ref, sems)
    fill_padded(pad_ref, g_ref, near_ref, far_ref, beside_ref, across_ref, 2)

    def first(r, _):
        zpad_ref[r] = smoothed_row(pad_ref, r + 1, smooth)
        return 0

    lax.fori_loop(0, rows + 2, first, 0, unroll=2)

    @pl.when(lax.axis_index("swath") == 0)
    def _():
        zpad_ref[0] = jnp.zeros_like(zpad_ref[0])

    @pl.when(lax.axis_index("swath") == lax.axis_size("swath") - 1)
    def _():
        zpad_ref[rows + 1] = jnp.zeros_like(zpad_ref[0])

    z_ref[...] = zpad_ref[1 : rows + 1, PAD : PAD + LON_DEV]

    def second(r, _):
        high, low = two_parts(smoothed_row(zpad_ref, r + 1, smooth)[PAD : PAD + LON_DEV])
        part_ref[r] = jnp.concatenate([high, low], axis=0)
        return 0

    lax.fori_loop(0, rows, second, 0, unroll=2)
    cells = lax.broadcasted_iota(jnp.int32, (LON_DEV, OBS_BLOCK), 0)

    def step(i, _):
        chunk_copy(jac_hbm, jac_ref, sems, i, GROUP * OBS_BLOCK, 0).wait()
        at = pl.ds(pl.multiple_of(i * GROUP, GROUP), GROUP)
        col = jnp.bitwise_and(col_ref[at], LON_DEV - 1)
        found = []
        for j in range(GROUP):
            line = i * GROUP + j
            jac = jac_ref[pl.ds(pl.multiple_of(line * OBS_BLOCK, OBS_BLOCK), OBS_BLOCK), :]
            got = dot(part_ref[row_ref[line]], jac, NT)
            both = got[:LON_DEV] + got[LON_DEV:]
            found.append(
                jnp.sum(jnp.where(cells == col[j : j + 1], both, 0.0), axis=0, keepdims=True)
            )
        image_ref[at] = jnp.concatenate(found, axis=0)
        return 0

    lax.fori_loop(0, lines // GROUP, step, 0, unroll=UNROLL)


def gram_kernel(
    share, cuts, smooth_ref, g_ref, near_ref, far_ref, beside_ref, across_ref, z_ref, w_ref,
    rb_ref, zb_ref, wb_ref, ub_ref, one_ref, two_ref, sum_ref, pad_ref,
):
    rows = g_ref.shape[0]
    smooth = smooth_ref[...]
    fill_padded(pad_ref, g_ref, near_ref, far_ref, beside_ref, across_ref, 1)

    def step(r, sums):
        z = z_ref[r]
        w = w_ref[r]
        v = smoothed_row(pad_ref, r + 1, smooth)[PAD : PAD + LON_DEV]
        made = []
        for total, (one, two) in zip(sums, ((z, z), (z, w), (w, w), (z, v), (w, v), (v, v))):
            made.append(total + jnp.sum((one * two).reshape(LON_DEV // 8, 8, LEV), axis=0))
        return tuple(made)

    zero = jnp.zeros((8, LEV), F32)
    zz, zw, ww, zv, wv, vv = lax.fori_loop(0, rows, step, (zero,) * 6)
    offset = 0
    for mask, size in cuts:
        offset = offset + (lax.axis_index("swath") // mask) % 2 * size
    own = pl.ds(offset, one_ref.shape[0])
    rb, zb, wb, ub = (ref[own] for ref in (rb_ref, zb_ref, wb_ref, ub_ref))
    vb = one_ref[...] + two_ref[...]
    lane = lax.broadcasted_iota(jnp.int32, (8, LANES), 1)
    sums = jnp.zeros((8, LANES), F32)
    pairs = (
        (zz, rb, rb), (zz, rb, zb), (zw, zb, wb), (zw, rb, wb), (ww, wb, ub),
        (ww, wb, wb), (wv, ub, vb), (zv, rb, vb), (wv, wb, vb), (vv, vb, vb),
    )
    for k, (state, one, two) in enumerate(pairs):
        both = state + jnp.sum(one * two, axis=0) * share
        both = jnp.sum(jnp.sum(both, axis=0, keepdims=True), axis=1, keepdims=True)
        sums = jnp.where(lane == k, both, sums)
    sum_ref[...] = jnp.broadcast_to(sums[None], sum_ref.shape)


def final_kernel(
    sum_ref, z_ref, w_ref, zm_ref, zo_ref, um_ref, uo_ref, x_ref, xb_ref, norm_ref
):
    sums = jnp.sum(sum_ref[...], axis=0)[:1]
    lane = lax.broadcasted_iota(jnp.int32, (1, LANES), 1)
    rr, rz, zw, rw, wu, ww, uv, rv, wv, vv = (
        jnp.sum(jnp.where(lane == k, sums, 0.0), axis=1, keepdims=True) for k in range(10)
    )
    grow = 1.0 / SHRINK
    first = rz / (zw * grow)
    big = first * grow
    rz_one = rz - 2.0 * big * zw + big * big * wu
    rr_one = rr - 2.0 * big * rw + big * big * ww
    ratio = rz_one / rz
    lift = 1.0 + ratio
    curve = lift * lift * (zw * grow) - 2.0 * lift * first * wu * (grow * grow) + big * big * uv
    second = rz_one / curve
    main = first + second * lift
    side = first * second * grow
    main_big = main * grow
    rr_two = (
        rr + main_big * main_big * ww + side * side * vv
        - 2.0 * main_big * rw + 2.0 * side * rv - 2.0 * main_big * side * wv
    )
    x_ref[...] = main[:, None] * z_ref[...] - side[:, None] * w_ref[...]
    half = zm_ref.shape[0]
    units = xb_ref.shape[1] // LANES
    for j in range(units):
        unit = lax.axis_index("chan") * units + j
        upper = (unit >= half).astype(jnp.int32)
        at = unit - upper * half
        here = upper == lax.axis_index("swath") % 2
        z_unit = jnp.where(here, zm_ref[at], zo_ref[at])
        u_unit = jnp.where(here, um_ref[at], uo_ref[at])
        xb_ref[:, j * LANES : (j + 1) * LANES] = main * z_unit - side * u_unit
    squares = jnp.where(lane == 0, rr, jnp.where(lane == 1, rr_one, rr_two))
    norm_ref[...] = jnp.sqrt(jnp.maximum(squares, 0.0))[:, : norm_ref.shape[1]]


def call(kernel, outs, scratch=(), flops=0, smem=(), hbm=(), limit=12 << 20, alias=None):
    shapes = [jax.ShapeDtypeStruct(s, d) for s, d in outs]

    def place_call(*args):
        count = len(args)
        far = [i % count for i in hbm]
        args = [
            pltpu.with_memory_space_constraint(a, pltpu.HBM) if i in far else a
            for i, a in enumerate(args)
        ]
        specs = [SMEM if i in smem else HBM if i in far else VMEM for i in range(count)]
        return pl.pallas_call(
            kernel,
            out_shape=shapes,
            in_specs=specs,
            out_specs=[VMEM] * len(shapes),
            scratch_shapes=list(scratch),
            input_output_aliases=alias or {},
            cost_estimate=pl.CostEstimate(flops=flops, transcendentals=0, bytes_accessed=1 << 20),
            compiler_params=pltpu.CompilerParams(vmem_limit_bytes=limit),
        )(*args)

    return place_call


def trade(value, axis, mask):
    size = lax.axis_size(axis)
    return lax.ppermute(value, axis, [(i, i ^ mask) for i in range(size)])


def powers(start, size):
    while start < size:
        yield start
        start *= 2


def add(one, two):
    return call(add_kernel, [(one.shape, F32)], limit=1 << 20)(one, two)[0]


def chips_sum(mine):
    parts = []
    for axis, start in (("swath", 2), ("chan", 1)):
        for m in powers(start, lax.axis_size(axis)):
            parts.append((axis, m))
    for axis, m in parts[:-1]:
        mine = add(mine, trade(mine, axis, m))
    axis, m = parts[-1]
    return mine, trade(mine, axis, m)


def chips_scatter(mine, got):
    parts = [("swath", m) for m in powers(2, lax.axis_size("swath"))]
    parts += [("chan", m) for m in powers(1, lax.axis_size("chan"))]
    cuts = []
    for axis, m in parts:
        units = mine.shape[0]
        if axis == "swath" and units % 2 == 0:
            half = (units // 2,) + mine.shape[1:]
            kernel = functools.partial(split_add_kernel, m)
            mine, sent = call(kernel, [(half, F32)] * 2, limit=1 << 20)(mine, got)
            cuts.append((m, units // 2))
        else:
            sent = mine = add(mine, got)
        got = trade(sent, axis, m)
    return (mine, got), cuts


def halos(g, near, far):
    bands, sectors = lax.axis_size("swath"), lax.axis_size("chan")
    rows, width = g.shape[0], near.shape[0]
    near = trade(near, "swath", 1)
    pairs = [(i, (i + 1) % bands) for i in range(1, bands, 2)]
    far = lax.ppermute(far, "swath", pairs + [(j, i) for i, j in pairs])
    edge = ((rows + 2 * width, width, LEV), F32)
    beside, across = call(edge_kernel, [edge, edge], limit=4 << 20)(g, near, far)
    beside = trade(beside, "chan", 1)
    pairs = [(i, (i + 1) % sectors) for i in range(1, sectors, 2)]
    across = lax.ppermute(across, "chan", pairs + [(j, i) for i, j in pairs])
    return g, near, far, beside, across


def body(
    innovations, obs_precision, jacobian, predictors, obs_column, obs_channel, obs_count,
    smoothing, bias_precision,
):
    slots = obs_precision.shape[0]
    lines = slots // OBS_BLOCK
    chunks = lines // GROUP
    owned = bias_precision.shape[1]
    bands, sectors = lax.axis_size("swath"), lax.axis_size("chan")
    channels = owned * sectors
    blocks = channels // CH_BLOCK
    units = channels // LANES
    smooth = smoothing.reshape(1, LEV)
    by_line = (lines, OBS_BLOCK)
    col = obs_column.reshape(by_line)
    channel = obs_channel.reshape(by_line)
    rows = col[:, 0] // LON_DEV
    tile = (LAT_DEV, LON_DEV, LEV)
    table = (units, NPRED, LANES)
    wide = LON_DEV + 2 * PAD
    acc = pltpu.VMEM((2 * NPRED * blocks, CH_BLOCK), F32)
    hot_flops = 2 * 2 * NPRED * blocks * CH_BLOCK * slots
    tile_flops = 4 * LON_DEV * LEV * slots
    line_out = (by_line, F32)
    line_f32 = pltpu.VMEM(by_line, F32)
    sems = lambda count: pltpu.SemaphoreType.DMA((count,))

    jac_space = [pltpu.VMEM((slots, LEV), BF16), sems(chunks)]

    half = (units // 2, NPRED, LANES)
    pair = (2,) + half
    first_bias = call(
        first_bias_kernel,
        [
            line_out, line_out, (pair, F32), (pair, F32), (table, F32), (by_line, jnp.int32),
            (by_line, jnp.int32), (predictors.shape, F32),
        ],
        [
            pltpu.VMEM((2,) + table, F32), pltpu.VMEM((4 * NPRED * blocks, CH_BLOCK), F32),
            line_f32, line_f32,
            pltpu.VMEM((NPRED, owned), F32), sems(5), sems(chunks),
        ],
        2 * hot_flops, (0,), range(1, 7),
    )
    bias = call(
        bias_kernel, [line_out, (half, F32), (half, F32)],
        [
            pltpu.VMEM(table, F32), acc, pltpu.VMEM((2 * NPRED * blocks, CH_BLOCK), BF16),
            pltpu.VMEM(table, F32),
        ],
        2 * hot_flops,
    )

    def adjoint(value, base, scale, width):
        kernel = functools.partial(adjoint_kernel, scale, base is not None, width, 0, chunks)
        args = (rows, value, col, jacobian) + (() if base is None else (base,))
        return call(
            kernel, [(tile, F32)] + [((width, LON_DEV, LEV), F32)] * 2, (), tile_flops, (0,),
            alias=None if base is None else {4: 0},
        )(*args)

    forward = lambda: call(
        forward_kernel, [line_out, (tile, F32)],
        [
            pltpu.VMEM((LAT_DEV + 4, wide, LEV), F32),
            pltpu.VMEM((LAT_DEV + 2, wide, LEV), F32),
            pltpu.VMEM((LAT_DEV, 2 * LON_DEV, LEV), BF16),
            *jac_space,
        ],
        tile_flops, (0,), (-1,),
    )

    source, weight, mine, other, prior, channel, col, pred = first_bias(
        obs_count, innovations.reshape(by_line), obs_precision.reshape(by_line),
        bias_precision, channel, col, predictors,
    )
    both = add(mine, trade(other, "swath", 1))
    g0 = adjoint(source, None, 1.0, 2)
    rb, diag, zb = call(first_ratio_kernel, [(half, F32)] * 3, limit=2 << 20)(*chips_sum(both))
    zo = trade(zb, "swath", 1)
    image, z = forward()(rows, smooth, *halos(*g0), col, jacobian)
    value, mine, other = bias(image, weight, prior, zb, zo, channel, pred)
    wb = add(mine, trade(other, "swath", 1))
    g1 = adjoint(value, g0[0], SHRINK, 2)
    wb, ub = call(ratio_kernel, [(half, F32)] * 2, limit=2 << 20)(*chips_sum(wb), diag)
    uo = trade(ub, "swath", 1)
    image, w = forward()(rows, smooth, *halos(*g1), col, jacobian)
    value, mine, other = bias(image, weight, prior, ub, uo, channel, pred)
    got = trade(other, "swath", 1)
    g2 = adjoint(value, g1[0], 1.0, 1)
    parts, cuts = chips_scatter(mine, got)
    copies = bands * sectors * parts[0].shape[0] // units
    gram = call(
        functools.partial(gram_kernel, 1.0 / copies, cuts), [((bands * sectors, 8, LANES), F32)],
        [pltpu.VMEM((LAT_DEV + 2, wide, LEV), F32)], 1 << 22,
    )
    sums = gram(smooth, *halos(*g2), z, w, rb, zb, wb, ub, *parts)[0]
    sums = lax.all_to_all(sums, ("swath", "chan"), 0, 0)
    x, xb, norms = call(
        final_kernel, [(tile, F32), ((NPRED, owned), F32), ((1, 3), F32)],
    )(sums, z, w, zb, zo, ub, uo)
    return x, xb, norms.reshape(3)


def solution(mesh):
    placed = (
        P(("swath", "chan")),
        P(("swath", "chan")),
        P(("swath", "chan"), None),
        P(None, ("swath", "chan")),
        P(("swath", "chan")),
        P(("swath", "chan")),
        P("swath", "chan"),
        P(),
        P(None, "chan"),
    )
    return jax.shard_map(
        body,
        mesh=mesh,
        in_specs=placed,
        out_specs=(P("swath", "chan", None), P(None, "chan"), P()),
        check_vma=False,
    )
```

```python
import functools
import jax
import jax.numpy as jnp
from jax import lax
from jax.experimental import pallas as pl
from jax.experimental.pallas import tpu as pltpu
from jax.sharding import PartitionSpec as P


LEV = 128
NPRED = 8
CH_BLOCK = 256
OBS_BLOCK = 128
LAT_DEV = 32
LON_DEV = 64
GROUP = 8
PAD = 8
UNROLL = 2
LANES = 128
SPLIT = CH_BLOCK // LANES
SHRINK = 2.0 ** -16
F32 = jnp.float32
BF16 = jnp.bfloat16
VMEM = pl.BlockSpec(memory_space=pltpu.VMEM)
SMEM = pl.BlockSpec(memory_space=pltpu.SMEM)
HBM = pl.BlockSpec(memory_space=pltpu.HBM)
NT = (((1,), (1,)), ((), ()))


def two_parts(value):
    high = value.astype(BF16)
    low = (value - high.astype(F32)).astype(BF16)
    return high, low


def dot(one, two, dims=(((1,), (0,)), ((), ()))):
    return lax.dot_general(one, two, dims, preferred_element_type=F32)


def channel_hot(channel):
    rows = lax.broadcasted_iota(jnp.int32, (CH_BLOCK, OBS_BLOCK), 0).astype(F32).astype(BF16)
    inner = jnp.bitwise_and(channel, CH_BLOCK - 1).astype(F32).astype(BF16)
    one, zero = jnp.ones_like(rows), jnp.zeros_like(rows)
    return jnp.concatenate(
        [jnp.where(rows == inner[line : line + 1], one, zero) for line in range(GROUP)], axis=1
    )


def flat_lines(value):
    return jnp.concatenate([value[line : line + 1] for line in range(GROUP)], axis=1)


def spread(terms, block_row, blocks):
    high, low = two_parts(terms)
    pieces = jnp.concatenate([high, low], axis=0)
    wide = jnp.broadcast_to(block_row, pieces.shape)
    zero = jnp.zeros_like(pieces)
    return jnp.concatenate(
        [jnp.where(wide == float(b), pieces, zero) for b in range(blocks)], axis=0
    )


def give_halves(full, mine_ref, other_ref):
    half = mine_ref.shape[0]
    odd = lax.axis_index("swath") % 2
    mine_ref[...] = full[pl.ds(odd * half, half)]
    other_ref[...] = full[pl.ds((1 - odd) * half, half)]


def put_table(out_ref, acc_ref, blocks, added):
    for b in range(blocks):
        low = 2 * NPRED * b
        total = acc_ref[low : low + NPRED] + acc_ref[low + NPRED : low + 2 * NPRED]
        for h in range(SPLIT):
            unit = SPLIT * b + h
            out_ref[unit] = total[:, h * LANES : (h + 1) * LANES] + added(unit)


def fetch(pairs, sems):
    copies = [pltpu.make_async_copy(a, b, sems.at[i]) for i, (a, b) in enumerate(pairs)]
    for copy in copies:
        copy.start()
    return copies


def chunk_copy(hbm_ref, ref, sems, i, size, axis):
    at = pl.ds(pl.multiple_of(i * size, size), size)
    where = at if axis == 0 else (slice(None), at)
    return pltpu.make_async_copy(hbm_ref.at[where], ref.at[where], sems.at[i])


def first_bias_kernel(
    count_ref, innov_hbm, prec_hbm, own_hbm, chan_hbm, col_hbm, pred_hbm,
    source_ref, weight_ref, mine_ref, other_ref, prior_ref, chan_ref, col_ref, pred_ref,
    both_ref, acc_ref, innov_ref, prec_ref, own_ref, sems, pred_sems,
):
    lines = innov_ref.shape[0]
    blocks = acc_ref.shape[0] // (4 * NPRED)
    wide_size = GROUP * OBS_BLOCK
    copies = fetch(
        [(chan_hbm, chan_ref), (innov_hbm, innov_ref), (prec_hbm, prec_ref), (own_hbm, own_ref)], sems
    )

    def start(i, _):
        chunk_copy(pred_hbm, pred_ref, pred_sems, i, wide_size, 1).start()
        return 0

    lax.fori_loop(0, lines // GROUP, start, 0)
    late = [pltpu.make_async_copy(col_hbm, col_ref, sems.at[4])]
    for copy in late:
        copy.start()
    acc_ref[...] = jnp.zeros_like(acc_ref)
    prior_ref[...] = jnp.zeros_like(prior_ref)
    for copy in copies:
        copy.wait()

    @pl.when(lax.axis_index("swath") == 0)
    def _():
        units = own_ref.shape[1] // LANES
        for j in range(units):
            prior_ref[lax.axis_index("chan") * units + j] = own_ref[:, j * LANES : (j + 1) * LANES]

    def step(i, _):
        chunk_copy(pred_hbm, pred_ref, pred_sems, i, wide_size, 1).wait()
        at = pl.ds(pl.multiple_of(i * GROUP, GROUP), GROUP)
        wide = pl.ds(pl.multiple_of(i * wide_size, wide_size), wide_size)
        slot = (
            (i * GROUP + lax.broadcasted_iota(jnp.int32, (GROUP, OBS_BLOCK), 0)) * OBS_BLOCK
            + lax.broadcasted_iota(jnp.int32, (GROUP, OBS_BLOCK), 1)
        )
        weight = jnp.where(slot < count_ref[0, 0], prec_ref[at], 0.0)
        source = weight * innov_ref[at]
        weight_ref[at] = weight
        source_ref[at] = source
        channel = chan_ref[at]
        hot = channel_hot(channel)
        block_row = flat_lines(lax.shift_right_logical(channel, 8).astype(F32)).astype(BF16)
        pred = pred_ref[:, wide]
        terms = spread(pred * flat_lines(source), block_row, blocks)
        squares = spread(pred * pred * flat_lines(weight), block_row, blocks)
        acc_ref[...] += dot(jnp.concatenate([terms, squares], axis=0), hot, NT)
        return 0

    lax.fori_loop(0, lines // GROUP, step, 0)
    put_table(both_ref.at[0], acc_ref, blocks, lambda unit: 0.0)
    put_table(both_ref.at[1], acc_ref.at[pl.ds(2 * NPRED * blocks, 2 * NPRED * blocks)], blocks, lambda unit: prior_ref[unit])
    for k in range(2):
        give_halves(both_ref.at[k], mine_ref.at[k], other_ref.at[k])
    for copy in late:
        copy.wait()


def bias_kernel(
    image_ref, weight_ref, prior_ref, mine_ref, other_ref, chan_ref, pred_ref,
    value_ref, keep_ref, send_ref, table_ref, acc_ref, look_ref, full_ref,
):
    lines = image_ref.shape[0]
    blocks = acc_ref.shape[0] // (2 * NPRED)
    wide_size = GROUP * OBS_BLOCK
    acc_ref[...] = jnp.zeros_like(acc_ref)
    half = mine_ref.shape[0]
    odd = lax.axis_index("swath") % 2
    full_ref[pl.ds(odd * half, half)] = mine_ref[...]
    full_ref[pl.ds((1 - odd) * half, half)] = other_ref[...]
    for b in range(blocks):
        coef = jnp.concatenate([full_ref[SPLIT * b + h] for h in range(SPLIT)], axis=1)
        high, low = two_parts(coef)
        look_ref[2 * NPRED * b : 2 * NPRED * (b + 1)] = jnp.concatenate([high, low], axis=0)

    def at(i):
        return pl.ds(pl.multiple_of(i * GROUP, GROUP), GROUP)

    def wide(i):
        return pl.ds(pl.multiple_of(i * wide_size, wide_size), wide_size)

    def block_of(channel):
        return flat_lines(lax.shift_right_logical(channel, 8).astype(F32))

    def look(i):
        channel = chan_ref[at(i)]
        pred = pred_ref[:, wide(i)]
        found = dot(look_ref[...], channel_hot(channel))
        block_wide = jnp.broadcast_to(block_of(channel), pred.shape)
        picked = jnp.zeros_like(pred)
        for b in range(blocks):
            low = 2 * NPRED * b
            both = found[low : low + NPRED] + found[low + NPRED : low + 2 * NPRED]
            picked = jnp.where(block_wide == float(b), both, picked)
        looked = jnp.sum(picked * pred, axis=0, keepdims=True)
        looked = jnp.concatenate(
            [looked[:, j * OBS_BLOCK : (j + 1) * OBS_BLOCK] for j in range(GROUP)], axis=0
        )
        value = weight_ref[at(i)] * (image_ref[at(i)] + looked)
        value_ref[at(i)] = value
        return value

    def tell(i, value):
        channel = chan_ref[at(i)]
        terms = pred_ref[:, wide(i)] * flat_lines(value)
        spreads = spread(terms, block_of(channel).astype(BF16), blocks)
        acc_ref[...] += dot(spreads, channel_hot(channel), NT)

    def step(i, value):
        following = look(i)
        tell(i - 1, value)
        return following

    last = lines // GROUP - 1
    tell(last, lax.fori_loop(1, last + 1, step, look(0), unroll=last))
    put_table(table_ref, acc_ref, blocks, lambda unit: prior_ref[unit] * full_ref[unit])
    give_halves(table_ref, keep_ref, send_ref)


def add_kernel(one_ref, two_ref, out_ref):
    out_ref[...] = one_ref[...] + two_ref[...]


def split_add_kernel(mask, one_ref, two_ref, keep_ref, send_ref):
    half = keep_ref.shape[0]
    bit = (lax.axis_index("swath") // mask) % 2
    keep, send = pl.ds(bit * half, half), pl.ds((1 - bit) * half, half)
    keep_ref[...] = one_ref[keep] + two_ref[keep]
    send_ref[...] = one_ref[send] + two_ref[send]


def first_ratio_kernel(one_ref, two_ref, r_ref, diag_ref, z_ref):
    r = one_ref[0] + two_ref[0]
    diag = one_ref[1] + two_ref[1]
    r_ref[...] = r
    diag_ref[...] = diag
    z_ref[...] = r / diag


def ratio_kernel(one_ref, two_ref, diag_ref, w_ref, u_ref):
    w = (one_ref[...] + two_ref[...]) * SHRINK
    w_ref[...] = w
    u_ref[...] = w / diag_ref[...]


def start_jac(jac_hbm, jac_ref, sems):
    def start(i, _):
        chunk_copy(jac_hbm, jac_ref, sems, i, GROUP * OBS_BLOCK, 0).start()
        return 0

    lax.fori_loop(0, jac_ref.shape[0] // (GROUP * OBS_BLOCK), start, 0)


def adjoint_kernel(scale, has_base, width, first, last, row_ref, value_ref, col_ref, jac_ref, *rest):
    out_ref = rest[-3] if width else rest[-1]
    if not has_base:
        out_ref[...] = jnp.zeros_like(out_ref)
    cells = lax.broadcasted_iota(jnp.int32, (LON_DEV, OBS_BLOCK), 0)

    def step(i, _):
        at = pl.ds(pl.multiple_of(i * GROUP, GROUP), GROUP)
        value = value_ref[at]
        high = value.astype(BF16).astype(F32)
        low = value - high
        col = jnp.bitwise_and(col_ref[at], LON_DEV - 1)
        for j in range(GROUP):
            hit = cells == col[j : j + 1]
            left = jnp.concatenate(
                [jnp.where(hit, high[j : j + 1], 0.0), jnp.where(hit, low[j : j + 1], 0.0)], axis=0
            ).astype(BF16)
            line = i * GROUP + j
            jac = jac_ref[pl.ds(pl.multiple_of(line * OBS_BLOCK, OBS_BLOCK), OBS_BLOCK), :]
            got = dot(left, jac)
            row = row_ref[line]
            out_ref[row] += got[:LON_DEV] + got[LON_DEV:]
        return 0

    lax.fori_loop(first, last, step, 0, unroll=2 * UNROLL)
    if scale != 1.0:
        out_ref[...] = out_ref[...] * scale
    if width:
        near_ref, far_ref = rest[-2:]
        odd = lax.axis_index("swath") % 2 == 1
        count = out_ref.shape[0]

        @pl.when(odd)
        def _():
            near_ref[...] = out_ref[:width]
            far_ref[...] = out_ref[count - width :]

        @pl.when(jnp.logical_not(odd))
        def _():
            near_ref[...] = out_ref[count - width :]
            far_ref[...] = out_ref[:width]

        band = lax.axis_index("swath")

        @pl.when((band == 0) | (band == lax.axis_size("swath") - 1))
        def _():
            far_ref[...] = jnp.zeros_like(far_ref)


def edge_kernel(g_ref, near_ref, far_ref, beside_ref, across_ref):
    rows, width = g_ref.shape[0], near_ref.shape[0]
    left, right = slice(0, width), slice(LON_DEV - width, LON_DEV)
    odd_band = lax.axis_index("swath") % 2 == 1
    odd_sector = lax.axis_index("chan") % 2 == 1

    def put(ref, cut):
        ref[width : width + rows] = g_ref[:, cut]

        @pl.when(odd_band)
        def _():
            ref[:width] = near_ref[:, cut]
            ref[width + rows :] = far_ref[:, cut]

        @pl.when(jnp.logical_not(odd_band))
        def _():
            ref[:width] = far_ref[:, cut]
            ref[width + rows :] = near_ref[:, cut]

    @pl.when(odd_sector)
    def _():
        put(beside_ref, left)
        put(across_ref, right)

    @pl.when(jnp.logical_not(odd_sector))
    def _():
        put(beside_ref, right)
        put(across_ref, left)


def fill_padded(pad_ref, g_ref, near_ref, far_ref, beside_ref, across_ref, width):
    rows = g_ref.shape[0]
    inside = slice(PAD, PAD + LON_DEV)
    above, below = slice(0, width), slice(width + rows, 2 * width + rows)
    west, east = slice(PAD - width, PAD), slice(PAD + LON_DEV, PAD + LON_DEV + width)
    pad_ref[width : width + rows, inside] = g_ref[...]
    odd_band = lax.axis_index("swath") % 2 == 1
    odd_sector = lax.axis_index("chan") % 2 == 1

    @pl.when(odd_band)
    def _():
        pad_ref[above, inside] = near_ref[...]
        pad_ref[below, inside] = far_ref[...]

    @pl.when(jnp.logical_not(odd_band))
    def _():
        pad_ref[above, inside] = far_ref[...]
        pad_ref[below, inside] = near_ref[...]

    @pl.when(odd_sector)
    def _():
        pad_ref[:, west] = beside_ref[...]
        pad_ref[:, east] = across_ref[...]

    @pl.when(jnp.logical_not(odd_sector))
    def _():
        pad_ref[:, west] = across_ref[...]
        pad_ref[:, east] = beside_ref[...]


def smoothed_row(pad_ref, row, smooth):
    here = pad_ref[row]
    size = here.shape[0]
    beside = (
        pad_ref[row - 1]
        + pad_ref[row + 1]
        + pltpu.roll(here, 1, 0)
        + pltpu.roll(here, size - 1, 0)
    )
    return here + smooth * (beside - 4.0 * here)


def forward_kernel(
    row_ref, smooth_ref, g_ref, near_ref, far_ref, beside_ref, across_ref, col_ref, jac_hbm,
    image_ref, z_ref, pad_ref, zpad_ref, part_ref, jac_ref, sems,
):
    rows = g_ref.shape[0]
    lines = col_ref.shape[0]
    smooth = smooth_ref[...]
    start_jac(jac_hbm, jac_ref, sems)
    fill_padded(pad_ref, g_ref, near_ref, far_ref, beside_ref, across_ref, 2)

    def first(r, _):
        zpad_ref[r] = smoothed_row(pad_ref, r + 1, smooth)
        return 0

    lax.fori_loop(0, rows + 2, first, 0, unroll=2)

    @pl.when(lax.axis_index("swath") == 0)
    def _():
        zpad_ref[0] = jnp.zeros_like(zpad_ref[0])

    @pl.when(lax.axis_index("swath") == lax.axis_size("swath") - 1)
    def _():
        zpad_ref[rows + 1] = jnp.zeros_like(zpad_ref[0])

    z_ref[...] = zpad_ref[1 : rows + 1, PAD : PAD + LON_DEV]

    def second(r, _):
        high, low = two_parts(smoothed_row(zpad_ref, r + 1, smooth)[PAD : PAD + LON_DEV])
        part_ref[r] = jnp.concatenate([high, low], axis=0)
        return 0

    lax.fori_loop(0, rows, second, 0, unroll=2)
    cells = lax.broadcasted_iota(jnp.int32, (LON_DEV, OBS_BLOCK), 0)

    def step(i, _):
        chunk_copy(jac_hbm, jac_ref, sems, i, GROUP * OBS_BLOCK, 0).wait()
        at = pl.ds(pl.multiple_of(i * GROUP, GROUP), GROUP)
        col = jnp.bitwise_and(col_ref[at], LON_DEV - 1)
        found = []
        for j in range(GROUP):
            line = i * GROUP + j
            jac = jac_ref[pl.ds(pl.multiple_of(line * OBS_BLOCK, OBS_BLOCK), OBS_BLOCK), :]
            got = dot(part_ref[row_ref[line]], jac, NT)
            both = got[:LON_DEV] + got[LON_DEV:]
            found.append(
                jnp.sum(jnp.where(cells == col[j : j + 1], both, 0.0), axis=0, keepdims=True)
            )
        image_ref[at] = jnp.concatenate(found, axis=0)
        return 0

    lax.fori_loop(0, lines // GROUP, step, 0, unroll=UNROLL)


def gram_kernel(
    share, cuts, smooth_ref, g_ref, near_ref, far_ref, beside_ref, across_ref, z_ref, w_ref,
    rb_ref, zb_ref, wb_ref, ub_ref, one_ref, two_ref, sum_ref, pad_ref,
):
    rows = g_ref.shape[0]
    smooth = smooth_ref[...]
    fill_padded(pad_ref, g_ref, near_ref, far_ref, beside_ref, across_ref, 1)

    def step(r, sums):
        z = z_ref[r]
        w = w_ref[r]
        v = smoothed_row(pad_ref, r + 1, smooth)[PAD : PAD + LON_DEV]
        made = []
        for total, (one, two) in zip(sums, ((z, z), (z, w), (w, w), (z, v), (w, v), (v, v))):
            made.append(total + jnp.sum((one * two).reshape(LON_DEV // 8, 8, LEV), axis=0))
        return tuple(made)

    zero = jnp.zeros((8, LEV), F32)
    zz, zw, ww, zv, wv, vv = lax.fori_loop(0, rows, step, (zero,) * 6)
    offset = 0
    for mask, size in cuts:
        offset = offset + (lax.axis_index("swath") // mask) % 2 * size
    own = pl.ds(offset, one_ref.shape[0])
    rb, zb, wb, ub = (ref[own] for ref in (rb_ref, zb_ref, wb_ref, ub_ref))
    vb = one_ref[...] + two_ref[...]
    lane = lax.broadcasted_iota(jnp.int32, (8, LANES), 1)
    sums = jnp.zeros((8, LANES), F32)
    pairs = (
        (zz, rb, rb), (zz, rb, zb), (zw, zb, wb), (zw, rb, wb), (ww, wb, ub),
        (ww, wb, wb), (wv, ub, vb), (zv, rb, vb), (wv, wb, vb), (vv, vb, vb),
    )
    for k, (state, one, two) in enumerate(pairs):
        both = state + jnp.sum(one * two, axis=0) * share
        both = jnp.sum(jnp.sum(both, axis=0, keepdims=True), axis=1, keepdims=True)
        sums = jnp.where(lane == k, both, sums)
    sum_ref[...] = jnp.broadcast_to(sums[:1][None], sum_ref.shape)


def final_kernel(
    sum_ref, z_ref, w_ref, zm_ref, zo_ref, um_ref, uo_ref, x_ref, xb_ref, norm_ref
):
    sums = jnp.sum(sum_ref[...], axis=0)
    lane = lax.broadcasted_iota(jnp.int32, (1, LANES), 1)
    rr, rz, zw, rw, wu, ww, uv, rv, wv, vv = (
        jnp.sum(jnp.where(lane == k, sums, 0.0), axis=1, keepdims=True) for k in range(10)
    )
    grow = 1.0 / SHRINK
    first = rz / (zw * grow)
    big = first * grow
    rz_one = rz - 2.0 * big * zw + big * big * wu
    rr_one = rr - 2.0 * big * rw + big * big * ww
    ratio = rz_one / rz
    lift = 1.0 + ratio
    curve = lift * lift * (zw * grow) - 2.0 * lift * first * wu * (grow * grow) + big * big * uv
    second = rz_one / curve
    main = first + second * lift
    side = first * second * grow
    main_big = main * grow
    rr_two = (
        rr + main_big * main_big * ww + side * side * vv
        - 2.0 * main_big * rw + 2.0 * side * rv - 2.0 * main_big * side * wv
    )
    x_ref[...] = main[:, None] * z_ref[...] - side[:, None] * w_ref[...]
    half = zm_ref.shape[0]
    units = xb_ref.shape[1] // LANES
    for j in range(units):
        unit = lax.axis_index("chan") * units + j
        upper = (unit >= half).astype(jnp.int32)
        at = unit - upper * half
        here = upper == lax.axis_index("swath") % 2
        z_unit = jnp.where(here, zm_ref[at], zo_ref[at])
        u_unit = jnp.where(here, um_ref[at], uo_ref[at])
        xb_ref[:, j * LANES : (j + 1) * LANES] = main * z_unit - side * u_unit
    squares = jnp.where(lane == 0, rr, jnp.where(lane == 1, rr_one, rr_two))
    norm_ref[...] = jnp.sqrt(jnp.maximum(squares, 0.0))[:, : norm_ref.shape[1]]


def call(kernel, outs, scratch=(), flops=0, smem=(), hbm=(), limit=12 << 20, alias=None):
    shapes = [jax.ShapeDtypeStruct(s, d) for s, d in outs]

    def place_call(*args):
        count = len(args)
        far = [i % count for i in hbm]
        args = [
            pltpu.with_memory_space_constraint(a, pltpu.HBM) if i in far else a
            for i, a in enumerate(args)
        ]
        specs = [SMEM if i in smem else HBM if i in far else VMEM for i in range(count)]
        return pl.pallas_call(
            kernel,
            out_shape=shapes,
            in_specs=specs,
            out_specs=[VMEM] * len(shapes),
            scratch_shapes=list(scratch),
            input_output_aliases=alias or {},
            cost_estimate=pl.CostEstimate(flops=flops, transcendentals=0, bytes_accessed=1 << 20),
            compiler_params=pltpu.CompilerParams(vmem_limit_bytes=limit),
        )(*args)

    return place_call


def trade(value, axis, mask):
    size = lax.axis_size(axis)
    return lax.ppermute(value, axis, [(i, i ^ mask) for i in range(size)])


def powers(start, size):
    while start < size:
        yield start
        start *= 2


def add(one, two):
    return call(add_kernel, [(one.shape, F32)], limit=1 << 20)(one, two)[0]


def chips_sum(mine):
    parts = []
    for axis, start in (("swath", 2), ("chan", 1)):
        for m in powers(start, lax.axis_size(axis)):
            parts.append((axis, m))
    for axis, m in parts[:-1]:
        mine = add(mine, trade(mine, axis, m))
    axis, m = parts[-1]
    return mine, trade(mine, axis, m)


def chips_scatter(mine, got):
    parts = [("swath", m) for m in powers(2, lax.axis_size("swath"))]
    parts += [("chan", m) for m in powers(1, lax.axis_size("chan"))]
    cuts = []
    for axis, m in parts:
        units = mine.shape[0]
        if axis == "swath" and units % 2 == 0:
            half = (units // 2,) + mine.shape[1:]
            kernel = functools.partial(split_add_kernel, m)
            mine, sent = call(kernel, [(half, F32)] * 2, limit=1 << 20)(mine, got)
            cuts.append((m, units // 2))
        else:
            sent = mine = add(mine, got)
        got = trade(sent, axis, m)
    return (mine, got), cuts


def halos(g, near, far):
    bands, sectors = lax.axis_size("swath"), lax.axis_size("chan")
    rows, width = g.shape[0], near.shape[0]
    near = trade(near, "swath", 1)
    pairs = [(i, (i + 1) % bands) for i in range(1, bands, 2)]
    far = lax.ppermute(far, "swath", pairs + [(j, i) for i, j in pairs])
    edge = ((rows + 2 * width, width, LEV), F32)
    beside, across = call(edge_kernel, [edge, edge], limit=4 << 20)(g, near, far)
    beside = trade(beside, "chan", 1)
    pairs = [(i, (i + 1) % sectors) for i in range(1, sectors, 2)]
    across = lax.ppermute(across, "chan", pairs + [(j, i) for i, j in pairs])
    return g, near, far, beside, across


def body(
    innovations, obs_precision, jacobian, predictors, obs_column, obs_channel, obs_count,
    smoothing, bias_precision,
):
    slots = obs_precision.shape[0]
    lines = slots // OBS_BLOCK
    chunks = lines // GROUP
    owned = bias_precision.shape[1]
    bands, sectors = lax.axis_size("swath"), lax.axis_size("chan")
    channels = owned * sectors
    blocks = channels // CH_BLOCK
    units = channels // LANES
    smooth = smoothing.reshape(1, LEV)
    by_line = (lines, OBS_BLOCK)
    col = obs_column.reshape(by_line)
    channel = obs_channel.reshape(by_line)
    rows = col[:, 0] // LON_DEV
    tile = (LAT_DEV, LON_DEV, LEV)
    table = (units, NPRED, LANES)
    wide = LON_DEV + 2 * PAD
    acc = pltpu.VMEM((2 * NPRED * blocks, CH_BLOCK), F32)
    hot_flops = 2 * 2 * NPRED * blocks * CH_BLOCK * slots
    tile_flops = 4 * LON_DEV * LEV * slots
    line_out = (by_line, F32)
    line_f32 = pltpu.VMEM(by_line, F32)
    sems = lambda count: pltpu.SemaphoreType.DMA((count,))

    jac_space = [pltpu.VMEM((slots, LEV), BF16), sems(chunks)]

    half = (units // 2, NPRED, LANES)
    pair = (2,) + half
    first_bias = call(
        first_bias_kernel,
        [
            line_out, line_out, (pair, F32), (pair, F32), (table, F32), (by_line, jnp.int32),
            (by_line, jnp.int32), (predictors.shape, F32),
        ],
        [
            pltpu.VMEM((2,) + table, F32), pltpu.VMEM((4 * NPRED * blocks, CH_BLOCK), F32),
            line_f32, line_f32,
            pltpu.VMEM((NPRED, owned), F32), sems(5), sems(chunks),
        ],
        2 * hot_flops, (0,), range(1, 7),
    )
    bias = call(
        bias_kernel, [line_out, (half, F32), (half, F32)],
        [
            pltpu.VMEM(table, F32), acc, pltpu.VMEM((2 * NPRED * blocks, CH_BLOCK), BF16),
            pltpu.VMEM(table, F32),
        ],
        2 * hot_flops,
    )

    def adjoint(value, base, scale, width):
        kernel = functools.partial(adjoint_kernel, scale, base is not None, width, 0, chunks)
        args = (rows, value, col, jacobian) + (() if base is None else (base,))
        return call(
            kernel, [(tile, F32)] + [((width, LON_DEV, LEV), F32)] * 2, (), tile_flops, (0,),
            alias=None if base is None else {4: 0},
        )(*args)

    forward = lambda: call(
        forward_kernel, [line_out, (tile, F32)],
        [
            pltpu.VMEM((LAT_DEV + 4, wide, LEV), F32),
            pltpu.VMEM((LAT_DEV + 2, wide, LEV), F32),
            pltpu.VMEM((LAT_DEV, 2 * LON_DEV, LEV), BF16),
            *jac_space,
        ],
        tile_flops, (0,), (-1,),
    )

    source, weight, mine, other, prior, channel, col, pred = first_bias(
        obs_count, innovations.reshape(by_line), obs_precision.reshape(by_line),
        bias_precision, channel, col, predictors,
    )
    both = add(mine, trade(other, "swath", 1))
    g0 = adjoint(source, None, 1.0, 2)
    rb, diag, zb = call(first_ratio_kernel, [(half, F32)] * 3, limit=2 << 20)(*chips_sum(both))
    zo = trade(zb, "swath", 1)
    image, z = forward()(rows, smooth, *halos(*g0), col, jacobian)
    value, mine, other = bias(image, weight, prior, zb, zo, channel, pred)
    wb = add(mine, trade(other, "swath", 1))
    g1 = adjoint(value, g0[0], SHRINK, 2)
    wb, ub = call(ratio_kernel, [(half, F32)] * 2, limit=2 << 20)(*chips_sum(wb), diag)
    uo = trade(ub, "swath", 1)
    image, w = forward()(rows, smooth, *halos(*g1), col, jacobian)
    value, mine, other = bias(image, weight, prior, ub, uo, channel, pred)
    got = trade(other, "swath", 1)
    g2 = adjoint(value, g1[0], 1.0, 1)
    parts, cuts = chips_scatter(mine, got)
    copies = bands * sectors * parts[0].shape[0] // units
    gram = call(
        functools.partial(gram_kernel, 1.0 / copies, cuts), [((bands * sectors, 1, LANES), F32)],
        [pltpu.VMEM((LAT_DEV + 2, wide, LEV), F32)], 1 << 22,
    )
    sums = gram(smooth, *halos(*g2), z, w, rb, zb, wb, ub, *parts)[0]
    sums = lax.all_to_all(sums, ("swath", "chan"), 0, 0)
    x, xb, norms = call(
        final_kernel, [(tile, F32), ((NPRED, owned), F32), ((1, 3), F32)],
    )(sums, z, w, zb, zo, ub, uo)
    return x, xb, norms.reshape(3)


def solution(mesh):
    placed = (
        P(("swath", "chan")),
        P(("swath", "chan")),
        P(("swath", "chan"), None),
        P(None, ("swath", "chan")),
        P(("swath", "chan")),
        P(("swath", "chan")),
        P("swath", "chan"),
        P(),
        P(None, "chan"),
    )
    return jax.shard_map(
        body,
        mesh=mesh,
        in_specs=placed,
        out_specs=(P("swath", "chan", None), P(None, "chan"), P()),
        check_vma=False,
    )
```
